32 devices in a mesh: tile: 8 (over z, x), mem: 4 (over y, core).
Axes of the slice: x: 2, y: 2, z: 4, core: 2. Of those that a mesh axis runs over, the one named last changes fastest.
Arguments:
- footprints: bfloat16 [1024, 128, 128], P('tile'), may hold values from -0.1875 to 0.1875
- tile_row: int32 [1024], P('tile'), may hold values from 0 to 127, as said below
- tile_col: int32 [1024], P('tile'), may hold values from 0 to 63, as said below
- prior_flux: bfloat16 [256, 8192], P('mem', 'tile'), may hold values from -12 to 12
- observed: float32 [256, 16384], P('mem', 'tile'), may hold values from -6 to 6
- precision_weight: int32 [16384], P('tile'), may hold values from 1 to 16
Outputs:
- gradient: float32 [256, 8192], P('mem', 'tile')
The draws below stay inside these ranges and needn't reach their ends.
Inputs may be any that keep to these rules, and one draw needn't show every extreme that they name: Among the 128 tiles of each index of tile, at most 24 have a row block of one owner (owner = tile_row // 16); in every draw one owner gets exactly 24 from every index. Likewise with owner = tile_col // 8: at most 24 from one index of tile to one owner, and one owner gets exactly 24 from every index.
All inputs are finite; a program needn't handle non-finite values.
Results may differ from the reference program's by a relative error of at most 0.0052.
Values may be sent and summed in bfloat16 or wider, within the bound.
No kernel may reach another device: no remote copies, remote signals or barrier semaphores. Data moves between devices by JAX's collectives and lax.ppermute only.
A program may use at most 64 MiB of HBM per device.

```python
import jax
import jax.numpy as jnp
from jax import lax

B = 128
MEMBERS = 256
TILE_DEV = 128
FLUX_DEV = 8
SOUND_DEV = 16
TILES = 1024
SOUNDINGS = 16384
N_TILE = 8


def spread_blocks(key, per_owner):
    capacity = TILE_DEV // N_TILE + max(1, TILE_DEV // (2 * N_TILE))
    slot_count = N_TILE * capacity
    key_perm, key_hot, key_local = jax.random.split(key, 3)
    hottest = jax.random.randint(key_hot, (), 0, N_TILE)
    key_list = jax.random.split(key_perm, N_TILE)
    ranking = jax.vmap(lambda random_subkey: jax.random.permutation(random_subkey, slot_count))(key_list)
    slot_owner = jnp.arange(slot_count) // capacity
    priority = ranking + slot_count * (slot_owner == hottest).astype(jnp.int32)[None, :]
    top_values, chosen = lax.top_k(priority, TILE_DEV)
    owners = chosen // capacity
    local_block = jax.random.randint(key_local, (N_TILE, TILE_DEV), 0, per_owner)
    return (owners * per_owner + local_block).reshape(-1).astype(jnp.int32)


def draw_tile_row(key, part):
    return spread_blocks(jax.random.fold_in(key, 11), SOUND_DEV)


def draw_tile_col(key, part):
    return spread_blocks(jax.random.fold_in(key, 23), FLUX_DEV)


def draw_prior_flux(key, part):
    key_center, key_noise = jax.random.split(jax.random.fold_in(key, 37))
    cells = FLUX_DEV * B * N_TILE
    background = 2.0 * jax.random.normal(key_center, (1, cells), jnp.float32)
    member_noise = jax.random.normal(key_noise, (MEMBERS, cells), jnp.float32)
    return jnp.clip(background + member_noise, -12.0, 12.0).astype(jnp.bfloat16)


def plant(array, rng, low, largest):
    extent = array.shape
    spot = [jax.random.randint(jax.random.fold_in(rng, axis), (), 0, extent[axis]) for axis in range(len(extent))]
    array = array.at[tuple(spot)].set(low)
    longest = extent.index(max(extent))
    spot[longest] = (spot[longest] + 1) % extent[longest]
    return array.at[tuple(spot)].set(largest)


def level_of(stream_key, shape, cuts, smallest, largest):
    level, own = 1.0, jax.random.fold_in(stream_key, 6)
    for dim, blocks in cuts:
        steps = jnp.exp(jax.random.uniform(jax.random.fold_in(own, dim), (blocks,), jnp.float32, smallest / len(cuts), largest / len(cuts)))
        level = level * jnp.repeat(steps, shape[dim] // blocks).reshape([-1 if axis == dim else 1 for axis in range(len(shape))])
    return level


def scatter_about(key, shape, scale, bound, shards=(), dtype=jnp.bfloat16):
    result = scale * jax.random.normal(key, shape, jnp.float32)
    if shards:
        result = result * level_of(key, shape, shards, -0.22, 0.18)
    return jnp.clip(result, -bound, bound).astype(dtype)


def setup_inputs(seed: int = 0) -> dict:
    key_of = jax.random.split(jax.random.key(seed), 7)
    return {
        "footprints": scatter_about(key_of[0], (TILES, B, B), (B * TILE_DEV // SOUND_DEV) ** -0.5, 0.1875, ((0, 8),)),
        "tile_row": draw_tile_row(jax.random.fold_in(key_of[6], 71), 0),
        "tile_col": draw_tile_col(jax.random.fold_in(key_of[6], 71), 0),
        "prior_flux": draw_prior_flux(jax.random.fold_in(key_of[6], 71), 0),
        "observed": scatter_about(key_of[4], (MEMBERS, SOUNDINGS), 1.0, 6.0, ((0, 4), (1, 8)), jnp.float32),
        "precision_weight": plant(jax.random.randint(key_of[5], (SOUNDINGS,), 1, 17), jax.random.fold_in(key_of[5], 1), 1, 16).astype(jnp.int32),
    }


def reference(footprints, tile_row, tile_col, prior_flux, observed, precision_weight):
    ensemble_mean = jnp.sum(prior_flux.astype(jnp.float32), axis=0, keepdims=True) / MEMBERS
    member_deviations = (prior_flux.astype(jnp.float32) - ensemble_mean).astype(jnp.bfloat16)
    flux_count = FLUX_DEV * N_TILE
    sound_blocks = SOUND_DEV * N_TILE
    flux_blocks = member_deviations.reshape(MEMBERS, flux_count, B).transpose(1, 0, 2)
    grouped = footprints.reshape(N_TILE, TILE_DEV, B, B)
    row_groups = tile_row.reshape(N_TILE, TILE_DEV).astype(jnp.int32)
    col_groups = tile_col.reshape(N_TILE, TILE_DEV).astype(jnp.int32)

    def forward(totals, inputs):
        footprint_block_grid, block_rows, block_cols = inputs
        retrieved_blocks = jnp.take(flux_blocks, block_cols, axis=0).astype(jnp.float32)
        tile_products = jnp.einsum("cuz,cdz->cud", retrieved_blocks, footprint_block_grid.astype(jnp.float32))
        return totals.at[block_rows].add(tile_products), None

    modelled = lax.scan(forward, jnp.zeros((sound_blocks, MEMBERS, B), jnp.float32), (grouped, row_groups, col_groups))[0]
    obs_blocks = observed.reshape(MEMBERS, sound_blocks, B).transpose(1, 0, 2)
    weight_factor = (precision_weight.astype(jnp.float32) / 8.0).reshape(sound_blocks, 1, B)
    weighted = (weight_factor * (modelled - obs_blocks)).astype(jnp.bfloat16)

    def backward(totals, inputs):
        footprint_block_grid, block_rows, block_cols = inputs
        retrieved_blocks = jnp.take(weighted, block_rows, axis=0).astype(jnp.float32)
        tile_products = jnp.einsum("bnh,bhd->bnd", retrieved_blocks, footprint_block_grid.astype(jnp.float32))
        return totals.at[block_cols].add(tile_products), None

    flux_totals = lax.scan(backward, jnp.zeros((flux_count, MEMBERS, B), jnp.float32), (grouped, row_groups, col_groups))[0]
    return flux_totals.transpose(1, 0, 2).reshape(MEMBERS, flux_count * B)
```

```python
import jax
import jax.numpy as jnp
from jax import lax
from jax.experimental import pallas as pl
from jax.experimental.pallas import tpu as pltpu
from jax.sharding import PartitionSpec as P


def rank_in_owner(owners):
    position = jnp.arange(owners.shape[0])
    earlier = (owners[:, None] == owners[None, :]) & (position[None, :] < position[:, None])
    return jnp.sum(earlier.astype(jnp.int32), axis=1)


def exchange(value, axis, distance):
    size = lax.axis_size(axis)
    return lax.ppermute(value, axis, [(i, i ^ distance) for i in range(size)])


def distances(size):
    found = []
    step = size // 2
    while step:
        found.append(step)
        step //= 2
    return found


def local_kernel(rows, cols, *refs, quarters, unroll):
    tiles = refs[:quarters]
    flux, observed, weight, near, far, modelled, weighted, total = refs[quarters:]
    soundings = modelled.shape[0] - 1
    cells = total.shape[0] - 1
    side = flux.shape[2]
    per_quarter = tiles[0].shape[0]
    modelled[...] = jnp.zeros_like(modelled)
    total[...] = jnp.zeros_like(total)

    for q in range(quarters):

        def forward(step, carry, q=q):
            terms = []
            for u in range(unroll):
                t = step * unroll + u
                c = jnp.minimum(cols[q * per_quarter + t], cells - 1)
                terms.append(
                    lax.dot_general(
                        flux[c], tiles[q][t], (((1,), (1,)), ((), ())), preferred_element_type=jnp.float32
                    )
                )
            for u in range(unroll):
                r = rows[q * per_quarter + step * unroll + u]
                modelled[r] = modelled[r] + terms[u]
            return carry

        lax.fori_loop(0, per_quarter // unroll, forward, 0)

    scale = weight[...].astype(jnp.float32) / 8.0
    for r in range(soundings):
        part = slice(r * side, (r + 1) * side)
        weighted[r] = (scale[:, part] * (modelled[r] - observed[:, part])).astype(jnp.bfloat16)
    weighted[soundings] = jnp.zeros_like(weighted[soundings])

    for q in range(quarters):

        def backward(step, carry, q=q):
            terms = []
            for u in range(unroll):
                t = step * unroll + u
                r = rows[q * per_quarter + t]
                terms.append(jnp.dot(weighted[r], tiles[q][t], preferred_element_type=jnp.float32))
            for u in range(unroll):
                c = cols[q * per_quarter + step * unroll + u]
                total[c] = total[c] + terms[u]
            return carry

        lax.fori_loop(0, per_quarter // unroll, backward, 0)

    half = cells // 2
    near[...] = total[:half]
    far[...] = total[half:cells].astype(jnp.bfloat16)


def body(footprints, tile_row, tile_col, prior_flux, observed, precision_weight):
    devices_tile = lax.axis_size("tile")
    devices_mem = lax.axis_size("mem")
    me = lax.axis_index("tile")
    quarter = lax.axis_index("mem")
    tile_count, side, _ = footprints.shape
    local_members = prior_flux.shape[0]
    members = local_members * devices_mem
    flux_local = prior_flux.shape[1] // side
    sound_local = observed.shape[1] // side
    flux_all = flux_local * devices_tile

    capacity = tile_count // devices_tile + max(1, tile_count // (2 * devices_tile))
    share = -(-capacity // devices_mem)
    capacity = share * devices_mem
    owner = tile_row // sound_local
    slot = owner * capacity + rank_in_owner(owner)
    hit = slot[None, :] == jnp.arange(devices_tile * capacity)[:, None]
    source = jnp.sum(jnp.where(hit, jnp.arange(tile_count)[None, :], 0), axis=1)
    code = (tile_row % sound_local) * flux_all + tile_col
    codes = jnp.sum(jnp.where(hit, code[None, :] + 1, 0), axis=1) - 1
    mine = lax.dynamic_slice_in_dim(source.reshape(devices_tile, capacity), quarter * share, share, axis=1)
    sent = jnp.take(footprints, mine.reshape(-1), axis=0)
    got = lax.all_to_all(sent, "tile", split_axis=0, concat_axis=0, tiled=True)
    got_codes = lax.all_to_all(
        codes.reshape(devices_tile, capacity), "tile", split_axis=0, concat_axis=0, tiled=True
    )
    quarters = [got]
    steps = distances(devices_mem)
    for distance in steps:
        quarters = quarters + [exchange(q, "mem", distance) for q in quarters]
    order = [0]
    for distance in steps:
        order = order + [q ^ distance for q in order]

    by_share = got_codes.reshape(devices_tile, devices_mem, share)
    table = jnp.stack([jnp.take(by_share, quarter ^ q, axis=1) for q in order]).reshape(-1)
    used = table >= 0
    col = jnp.where(used, table % flux_all, 0)
    relative = (col // flux_local) ^ me
    place = jnp.zeros_like(relative)
    for i, distance in enumerate(distances(devices_tile)):
        place = place + (((relative // distance) & 1) << i)
    rows = jnp.where(used, table // flux_all, sound_local)
    cols = jnp.where(used, place * flux_local + col % flux_local, flux_all)

    prior = prior_flux.astype(jnp.float32)
    total = jnp.sum(prior, axis=0, keepdims=True)
    for distance in reversed(distances(devices_mem)):
        total = total + exchange(total, "mem", distance)
    anomalies = (prior - total / members).astype(jnp.bfloat16)
    flux = anomalies.reshape(local_members, flux_local, side).transpose(1, 0, 2)
    for distance in distances(devices_tile):
        flux = jnp.concatenate([flux, exchange(flux, "tile", distance)], axis=0)

    unroll = 8
    while got.shape[0] % unroll:
        unroll //= 2
    vmem = pl.BlockSpec(memory_space=pltpu.VMEM)
    smem = pl.BlockSpec(memory_space=pltpu.SMEM)
    near, far = pl.pallas_call(
        lambda *refs: local_kernel(*refs, quarters=devices_mem, unroll=unroll),
        out_shape=(
            jax.ShapeDtypeStruct((flux_all // 2, local_members, side), jnp.float32),
            jax.ShapeDtypeStruct((flux_all // 2, local_members, side), jnp.bfloat16),
        ),
        in_specs=[smem, smem] + [vmem] * (devices_mem + 3),
        out_specs=(vmem, vmem),
        scratch_shapes=[
            pltpu.VMEM((sound_local + 1, local_members, side), jnp.float32),
            pltpu.VMEM((sound_local + 1, local_members, side), jnp.bfloat16),
            pltpu.VMEM((flux_all + 1, local_members, side), jnp.float32),
        ],
        name="local_adjoint",
    )(rows, cols, *quarters, flux, observed, precision_weight.reshape(1, -1))

    for distance in reversed(distances(devices_tile)):
        near = near + exchange(far, "tile", distance).astype(jnp.float32)
        if distance < devices_tile // 2:
            half = near.shape[0] // 2
            near, far = near[:half], near[half:].astype(jnp.bfloat16)
    return near.transpose(1, 0, 2).reshape(local_members, flux_local * side)


def solution(mesh):
    in_specs = (
        P("tile", None, None),
        P("tile"),
        P("tile"),
        P("mem", "tile"),
        P("mem", "tile"),
        P("tile"),
    )
    return jax.shard_map(body, mesh=mesh, in_specs=in_specs, out_specs=P("mem", "tile"), check_vma=False)
```

```python
import jax
import jax.numpy as jnp
from jax import lax
from jax.experimental import pallas as pl
from jax.experimental.pallas import tpu as pltpu
from jax.sharding import PartitionSpec as P

CHUNKS = 2


def rank_in_owner(owners):
    position = jnp.arange(owners.shape[0])
    earlier = (owners[:, None] == owners[None, :]) & (position[None, :] < position[:, None])
    return jnp.sum(earlier.astype(jnp.int32), axis=1)


def exchange(value, axis, distance):
    size = lax.axis_size(axis)
    return lax.ppermute(value, axis, [(i, i ^ distance) for i in range(size)])


def distances(size):
    found = []
    step = 1
    while step < size:
        found.append(step)
        step *= 2
    return found


def routes(size):
    first = distances(size)
    second = list(first)
    if len(second) > 1:
        second[0], second[1] = second[1], second[0]
    return first, second


def listed(relative, route):
    place = jnp.zeros_like(relative)
    for i, distance in enumerate(reversed(route)):
        place = place + (((relative // distance) & 1) << i)
    return place


def gather_pieces(value, route):
    pieces = [value]
    held = value
    for i, distance in enumerate(reversed(route)):
        pieces.append(exchange(held, "tile", distance))
        if i + 1 < len(route):
            held = jnp.concatenate([held, pieces[-1]], axis=0)
    return pieces


def load_flux(flux, pieces, piece_rows):
    cells, members, side = flux.shape
    half = cells // 2
    at = 0
    for refs, rows in zip(pieces, piece_rows):
        count = half // sum(ref.shape[0] // rows for ref in refs)
        for ref in refs:
            for l in range(ref.shape[0] // rows):
                flux[at : at + count] = ref[l * rows : l * rows + count * members].reshape(count, members, side)
                at += count


def run_forward(rows, cols, base, tiles, flux, modelled, unroll):
    cells = flux.shape[0]

    def step(i, carry):
        terms = []
        for u in range(unroll):
            t = i * unroll + u
            c = jnp.minimum(cols[base + t], cells - 1)
            terms.append(
                lax.dot_general(flux[c], tiles[t], (((1,), (1,)), ((), ())), preferred_element_type=jnp.float32)
            )
        for u in range(unroll):
            r = rows[base + i * unroll + u]
            modelled[r] = modelled[r] + terms[u]
        return carry

    lax.fori_loop(0, tiles.shape[0] // unroll, step, 0)


def run_backward(rows, cols, base, tiles, weighted, total, unroll):
    def step(i, carry):
        terms = []
        for u in range(unroll):
            t = i * unroll + u
            terms.append(jnp.dot(weighted[rows[base + t]], tiles[t], preferred_element_type=jnp.float32))
        for u in range(unroll):
            c = cols[base + i * unroll + u]
            total[c] = total[c] + terms[u]
        return carry

    lax.fori_loop(0, tiles.shape[0] // unroll, step, 0)


def forward_kernel(rows, cols, *refs, buffers, piece_rows, base, unroll):
    tiles, refs = refs[:buffers], refs[buffers:]
    count = (len(refs) - 2) // 2
    modelled, flux = refs[-2:]
    load_flux(flux, (refs[:count], refs[count : 2 * count]), piece_rows)
    modelled[...] = jnp.zeros_like(modelled)
    for b in range(buffers):
        run_forward(rows, cols, base + b * tiles[b].shape[0], tiles[b], flux, modelled, unroll)


def adjoint_kernel(rows, cols, *refs, buffers, new, carried, pieces, piece_rows, unroll):
    tiles, refs = refs[:buffers], refs[buffers:]
    groups, refs = (refs[:pieces], refs[pieces : 2 * pieces]), refs[2 * pieces :]
    if carried:
        earlier, refs = refs[0], refs[1:]
    observed, weight, near_a, far_a, near_b, far_b, modelled, weighted, total, flux = refs
    soundings = modelled.shape[0] - 1
    cells = flux.shape[0]
    side = flux.shape[2]
    per_buffer = tiles[0].shape[0]
    load_flux(flux, groups, piece_rows)
    if carried:
        modelled[...] = earlier[...]
    else:
        modelled[...] = jnp.zeros_like(modelled)
    total[...] = jnp.zeros_like(total)
    for b in range(buffers - new, buffers):
        run_forward(rows, cols, b * per_buffer, tiles[b], flux, modelled, unroll)
    scale = weight[...].astype(jnp.float32) / 8.0
    for r in range(soundings):
        part = slice(r * side, (r + 1) * side)
        weighted[r] = (scale[:, part] * (modelled[r] - observed[:, part])).astype(jnp.bfloat16)
    weighted[soundings] = jnp.zeros_like(weighted[soundings])
    for b in range(buffers):
        run_backward(rows, cols, b * per_buffer, tiles[b], weighted, total, unroll)
    quarter = cells // 4
    near_a[...] = total[:quarter]
    far_a[...] = total[quarter : 2 * quarter].astype(jnp.bfloat16)
    near_b[...] = total[2 * quarter : 3 * quarter]
    far_b[...] = total[3 * quarter : cells].astype(jnp.bfloat16)


def body(footprints, tile_row, tile_col, prior_flux, observed, precision_weight):
    devices_tile = lax.axis_size("tile")
    devices_mem = lax.axis_size("mem")
    me = lax.axis_index("tile")
    quarter = lax.axis_index("mem")
    tile_count, side, _ = footprints.shape
    local_members = prior_flux.shape[0]
    members = local_members * devices_mem
    flux_local = prior_flux.shape[1] // side
    half_local = flux_local // 2
    sound_local = observed.shape[1] // side
    flux_all = flux_local * devices_tile
    route_a, route_b = routes(devices_tile)

    capacity = tile_count // devices_tile + max(1, tile_count // (2 * devices_tile))
    share = -(-capacity // devices_mem)
    chunks = CHUNKS if share % CHUNKS == 0 else 1
    part = share // chunks
    capacity = share * devices_mem
    owner = tile_row // sound_local
    slot = owner * capacity + rank_in_owner(owner)
    wanted = (
        jnp.arange(devices_tile)[None, :, None] * capacity
        + quarter * share
        + jnp.arange(chunks)[:, None, None] * part
        + jnp.arange(part)[None, None, :]
    ).reshape(-1)
    hit = slot[None, :] == wanted[:, None]
    source = jnp.sum(jnp.where(hit, jnp.arange(tile_count)[None, :], 0), axis=1).reshape(chunks, -1)
    received = [
        lax.all_to_all(
            jnp.take(footprints, source[k], axis=0, mode="clip"), "tile", split_axis=0, concat_axis=0, tiled=True
        )
        for k in range(chunks)
    ]

    prior = prior_flux.astype(jnp.float32)
    mean = jnp.sum(prior, axis=0, keepdims=True)
    for distance in distances(devices_mem):
        mean = mean + exchange(mean, "mem", distance)
    anomalies = (prior - mean / members).astype(jnp.bfloat16)
    blocks = anomalies.reshape(local_members, flux_local, side).transpose(1, 0, 2).reshape(-1, side)

    digits = jnp.stack([tile_row % 128, tile_row // 128, tile_col % 128, tile_col // 128])
    digit_rows = -(-digits.size // side)
    digit_rows += -digit_rows % 16
    digits = jnp.pad(digits.reshape(-1), (0, digit_rows * side - digits.size)).reshape(digit_rows, side)
    half_rows = half_local * local_members
    rows_a = half_rows + digit_rows
    pieces_a = gather_pieces(
        jnp.concatenate([blocks[:half_rows], digits.astype(jnp.bfloat16)], axis=0), route_a
    )
    pieces_b = gather_pieces(blocks[half_rows:], route_b)

    listed_digits = jnp.concatenate(
        [p.reshape(-1, rows_a, side)[:, half_rows:] for p in pieces_a], axis=0
    ).reshape(devices_tile, -1)[:, : 4 * tile_count]
    places = listed(jnp.arange(devices_tile) ^ me, route_a)
    chosen = places[:, None] == jnp.arange(devices_tile)[None, :]
    ids = jnp.sum(jnp.where(chosen[:, :, None], listed_digits.astype(jnp.float32)[None], 0.0), axis=1)
    ids = ids.astype(jnp.int32).reshape(devices_tile, 4, tile_count)
    row = ids[:, 0] + 128 * ids[:, 1]
    col = ids[:, 2] + 128 * ids[:, 3]
    here = row // sound_local == me
    position = jnp.arange(tile_count)
    before = jnp.sum(
        (here[:, None, :] & (position[None, None, :] < position[None, :, None])).astype(jnp.int32), axis=2
    )
    relative = (col // flux_local) ^ me
    inner = col % flux_local
    upper = inner // half_local
    place = (
        upper * (flux_all // 2)
        + jnp.where(upper == 0, listed(relative, route_a), listed(relative, route_b)) * half_local
        + inner % half_local
    )
    code = (row % sound_local) * flux_all + place + 1
    order = [0]
    for distance in reversed(distances(devices_mem)):
        order = order + [q ^ distance for q in order]
    wanted = (
        (quarter ^ jnp.array(order))[None, :, None, None] * share
        + jnp.arange(chunks)[:, None, None, None] * part
        + jnp.arange(part)[None, None, None, :]
        + jnp.zeros((chunks, devices_mem, devices_tile, part), jnp.int32)
    )
    found = here[None, None, :, None, :] & (before[None, None, :, None, :] == wanted[..., None])
    table = jnp.sum(jnp.where(found, code[None, None, :, None, :], 0), axis=-1).reshape(-1) - 1
    rows = jnp.where(table >= 0, table // flux_all, sound_local)
    cols = jnp.where(table >= 0, table % flux_all, flux_all)

    buffers = []
    for k in range(chunks):
        held = [received[k]]
        for distance in reversed(distances(devices_mem)):
            held = held + [exchange(q, "mem", distance) for q in held]
        buffers.append(held)

    per_buffer = received[0].shape[0]
    unroll = 8
    while per_buffer % unroll:
        unroll //= 2
    vmem = pl.BlockSpec(memory_space=pltpu.VMEM)
    smem = pl.BlockSpec(memory_space=pltpu.SMEM)
    pieces = list(pieces_a) + list(pieces_b)
    piece_rows = (rows_a, half_rows)
    flux_scratch = pltpu.VMEM((flux_all, local_members, side), jnp.bfloat16)
    modelled_shape = (sound_local + 1, local_members, side)
    early = []
    if chunks > 1:
        old = [b for held in buffers[:-1] for b in held]
        early = [
            pl.pallas_call(
                lambda *refs: forward_kernel(
                    *refs, buffers=len(old), piece_rows=piece_rows, base=0, unroll=unroll
                ),
                out_shape=jax.ShapeDtypeStruct(modelled_shape, jnp.float32),
                in_specs=[smem, smem] + [vmem] * (len(old) + len(pieces)),
                out_specs=vmem,
                scratch_shapes=[flux_scratch],
                name="forward",
            )(rows, cols, *old, *pieces)
        ]
    tiles = [b for held in buffers for b in held]
    quarter_shape = (flux_all // 4, local_members, side)
    near_a, far_a, near_b, far_b = pl.pallas_call(
        lambda *refs: adjoint_kernel(
            *refs,
            buffers=len(tiles),
            new=devices_mem,
            carried=bool(early),
            pieces=len(pieces_a),
            piece_rows=piece_rows,
            unroll=unroll,
        ),
        out_shape=(
            jax.ShapeDtypeStruct(quarter_shape, jnp.float32),
            jax.ShapeDtypeStruct(quarter_shape, jnp.bfloat16),
        )
        * 2,
        in_specs=[smem, smem] + [vmem] * (len(tiles) + len(pieces) + len(early) + 2),
        out_specs=(vmem,) * 4,
        scratch_shapes=[
            pltpu.VMEM(modelled_shape, jnp.float32),
            pltpu.VMEM(modelled_shape, jnp.bfloat16),
            pltpu.VMEM((flux_all + 1, local_members, side), jnp.float32),
            flux_scratch,
        ],
        name="adjoint",
    )(rows, cols, *tiles, *pieces, *early, observed, precision_weight.reshape(1, -1))

    sums = []
    for near, far, route in ((near_a, far_a, route_a), (near_b, far_b, route_b)):
        for i, distance in enumerate(route):
            near = near + exchange(far, "tile", distance).astype(jnp.float32)
            if i + 1 < len(route):
                half = near.shape[0] // 2
                near, far = near[:half], near[half:].astype(jnp.bfloat16)
        sums.append(near)
    gradient = jnp.concatenate(sums, axis=0)
    return gradient.transpose(1, 0, 2).reshape(local_members, flux_local * side)


def solution(mesh):
    in_specs = (
        P("tile", None, None),
        P("tile"),
        P("tile"),
        P("mem", "tile"),
        P("mem", "tile"),
        P("tile"),
    )
    return jax.shard_map(body, mesh=mesh, in_specs=in_specs, out_specs=P("mem", "tile"), check_vma=False)
```
